32 devices in a mesh: mem: 8 (over y, x, core), sub: 4 (over z).
Axes of the slice: x: 2, y: 2, z: 4, core: 2. Of those that a mesh axis runs over, the one named last changes fastest.
Arguments:
- control: bfloat16 [64, 1024, 128], P('mem', 'sub'), may hold values from -6 to 6
- perturb: bfloat16 [64, 1024, 128], P('mem', 'sub'), may hold values from -6 to 6
- obs_column: int32 [8, 4, 1024], P('mem', 'sub'), may hold values from 0 to 255
- obs_count: int32 [8, 4], P('mem', 'sub'), may hold values from 128 to 1024, as said below
- obs_background: bfloat16 [8, 4, 1024, 128], P('mem', 'sub'), may hold values from -6 to 6
- obs_value: bfloat16 [8, 4, 1024, 128], P('mem', 'sub'), may hold values from -6 to 6
- obs_weight: float32 [8, 4, 1024], P('mem', 'sub'), may hold values from 0.05 to 0.5
- w_in: bfloat16 [128, 2048], replicated, may hold values from -0.5 to 0.5
- b_in: float32 [2048], replicated, may hold values from -3 to 3
- w_out: bfloat16 [2048, 128], replicated, may hold values from -0.125 to 0.125
Outputs:
- increment: float32 [1024, 128], P(('sub', 'mem'))
- grad_columns: float32 [1024, 128], P(('sub', 'mem'))
The draws below stay inside these ranges and needn't reach their ends.
Inputs may be any that keep to these rules, and one draw needn't show every extreme that they name: `obs_count`: at least one batch has all 1024 slots live in every draw.
All inputs are finite; a program needn't handle non-finite values.
Results may differ from the reference program's by a relative error of at most 0.0025.
Values sent between devices are 32-bit elements; how exact they have to be, the bound alone decides.
No kernel may reach another device: no remote copies, remote signals or barrier semaphores. Data moves between devices by JAX's collectives and lax.ppermute only.
A program may use at most 64 MiB of HBM per device.

```python
import math
import jax
import jax.numpy as jnp
from jax import lax

LEV = 128
HID = 2048
NOUT = 128
CDEV = 256
OBS_CAP = 1024
SWEEPS = 4
MEMBERS = 64
COLS = 1024
N_MEM = 8
N_SUB = 4


def draw_obs_count(key, part):
    first_key = jax.random.fold_in(key, 11)
    second_key = jax.random.fold_in(key, 23)
    counts = jax.random.randint(first_key, (N_MEM * N_SUB,), OBS_CAP // 8, OBS_CAP + 1)
    chosen = jax.random.randint(second_key, (), 0, N_MEM * N_SUB)
    counts = counts.at[chosen].set(OBS_CAP)
    return counts.reshape(N_MEM, N_SUB).astype(jnp.int32)


def touch_ends(entries, own_key, low, top_value):
    dims = entries.shape
    spot = [jax.random.randint(jax.random.fold_in(own_key, axis), (), 0, dims[axis]) for axis in range(len(dims))]
    entries = entries.at[tuple(spot)].set(low)
    longest = dims.index(max(dims))
    spot[longest] = (spot[longest] + 1) % dims[longest]
    return entries.at[tuple(spot)].set(top_value)


def shard_levels(key, shape, pieces, smallest, high):
    loudness = 1.0
    for position, parts in pieces:
        heights = jax.random.uniform(jax.random.fold_in(jax.random.fold_in(key, 6), position), (parts,), jnp.float32, smallest / len(pieces), high / len(pieces))
        loudness = loudness * jnp.repeat(jnp.exp(heights), shape[position] // parts).reshape((-1,) + (1,) * (len(shape) - 1 - position))
    return loudness


def noise(rng, shape, deviation, limit, cuts=(), held_as=jnp.bfloat16):
    result = jax.random.normal(rng, shape, jnp.float32) * deviation
    if len(cuts) > 0:
        result = shard_levels(rng, shape, cuts, -0.22, 0.18) * result
    return jnp.clip(result, min=-limit, max=limit).astype(held_as)


def setup_inputs(seed: int = 0) -> dict:
    key_list = jax.random.split(jax.random.key(seed), 11)
    control = noise(key_list[0], (MEMBERS, COLS, LEV), 1.0, 6.0, ((0, 8), (1, 4)))
    perturb = noise(key_list[1], (MEMBERS, COLS, LEV), 1.0, 6.0, ((0, 8), (1, 4)))
    obs_column = touch_ends(jax.random.randint(key_list[2], (N_MEM, N_SUB, OBS_CAP), 0, CDEV), jax.random.fold_in(key_list[2], 1), 0, CDEV - 1).astype(jnp.int32)
    obs_count = draw_obs_count(jax.random.fold_in(key_list[10], 71), 0)
    obs_background = noise(key_list[4], (N_MEM, N_SUB, OBS_CAP, LEV), 1.0, 6.0, ((0, 8), (1, 4)))
    obs_value = noise(key_list[5], (N_MEM, N_SUB, OBS_CAP, NOUT), 1.0, 6.0, ((0, 8), (1, 4)))
    obs_weight = jnp.clip(jnp.exp(math.log(0.5) - 2.3025851 * jax.random.uniform(key_list[6], (N_MEM, N_SUB, OBS_CAP), jnp.float32) ** shard_levels(key_list[6], (N_MEM, N_SUB, OBS_CAP), ((0, 8), (1, 4)), -0.2, 0.2)), 0.05, 0.5)
    w_in = noise(key_list[7], (LEV, HID), LEV ** -0.5, 0.5)
    b_in = noise(key_list[8], (HID,), 0.5, 3.0, (), jnp.float32)
    w_out = noise(key_list[9], (HID, NOUT), HID ** -0.5, 0.125)
    return dict(control=control, perturb=perturb, obs_column=obs_column, obs_count=obs_count, obs_background=obs_background, obs_value=obs_value, obs_weight=obs_weight, w_in=w_in, b_in=b_in, w_out=w_out)


diffusion = 0.4

def gelu_tanh(values):
    return jax.nn.gelu(values, approximate=True)

def observe(sampled, live, background, targets, weights, w_in, b_in, w_out):
    inputs = (background.astype(jnp.float32) + sampled).astype(jnp.bfloat16)
    hidden_pre = jnp.dot(inputs, w_in, preferred_element_type=jnp.float32) + b_in
    hidden, pullback = jax.vjp(gelu_tanh, hidden_pre)
    hidden_low = hidden.astype(jnp.bfloat16)
    outputs = jnp.dot(hidden_low, w_out, preferred_element_type=jnp.float32)
    misfit = ((outputs - targets.astype(jnp.float32)) * (weights * live)[:, None]).astype(jnp.bfloat16)
    back_hidden = lax.dot_general(misfit, w_out, (((1,), (1,)), ((), ())), preferred_element_type=jnp.float32)
    back_pre, = pullback(back_hidden)
    back_pre = back_pre.astype(jnp.bfloat16)
    back_input = lax.dot_general(back_pre, w_in, (((1,), (1,)), ((), ())), preferred_element_type=jnp.float32)
    return back_input.astype(jnp.bfloat16)

def smooth(field):
    for sweep_index in range(SWEEPS):
        field = field + diffusion * (jnp.roll(field, 1, 0) - 2.0 * field + jnp.roll(field, -1, 0))
    return field

def reference(control, perturb, obs_column, obs_count, obs_background, obs_value, obs_weight, w_in, b_in, w_out):

    def add_member(running, pair):
        member_control, member_perturb = pair
        localized = smooth(member_control.astype(jnp.float32))
        return (running + localized * member_perturb.astype(jnp.float32), None)
    summed, unused = lax.scan(add_member, jnp.zeros((COLS, LEV), jnp.float32), (control, perturb))
    increment = summed * (MEMBERS - 1) ** (-0.5)
    offsets = (jnp.arange(N_SUB, dtype=jnp.int32) * CDEV).astype(jnp.int32)
    global_cols = (obs_column + offsets[None, :, None]).astype(jnp.int32).reshape(N_MEM * N_SUB, OBS_CAP)
    slots = jnp.arange(OBS_CAP, dtype=jnp.int32)
    live = (slots[None, None, :] < obs_count[:, :, None]).astype(jnp.float32).reshape(N_MEM * N_SUB, OBS_CAP)
    backgrounds = obs_background.reshape(N_MEM * N_SUB, OBS_CAP, LEV)
    targets = obs_value.reshape(N_MEM * N_SUB, OBS_CAP, NOUT)
    weights = obs_weight.reshape(N_MEM * N_SUB, OBS_CAP)

    def one_batch(items):
        cols_here, live_here, back_here, target_here, weight_here = items
        sampled = jnp.take(increment, cols_here, axis=0)
        return observe(sampled, live_here, back_here, target_here, weight_here, w_in, b_in, w_out)
    back_inputs = lax.map(one_batch, (global_cols, live, backgrounds, targets, weights))
    grad_columns = jnp.zeros((COLS, LEV), jnp.float32).at[global_cols.reshape(-1)].add(back_inputs.reshape(-1, LEV).astype(jnp.float32))
    return (increment, grad_columns)
```

```python
import jax
import jax.numpy as jnp
from jax import lax
from jax.sharding import PartitionSpec as P

SWEEPS = 4


diffusion = 0.4


def padded_2(block, sides, width):
    for axis, dim in sides:
        count = lax.axis_size(axis)
        forward = [(i, i + 1) for i in range(count - 1)]
        forward.append((count - 1, 0))
        backward = [(target, source) for source, target in forward]
        low = lax.ppermute(
            lax.slice_in_dim(block, block.shape[dim] - width, None, axis=dim), axis, forward
        )
        high = lax.ppermute(lax.slice_in_dim(block, 0, width, axis=dim), axis, backward)
        block = jnp.concatenate([low, block, high], axis=dim)
    return block


def gelu_tanh(values):
    return jax.nn.gelu(values, approximate=True)


def sweep(padded):
    middle = padded[:, 1:-1]
    return middle + diffusion * (padded[:, :-2] - 2.0 * middle + padded[:, 2:])


def bit_swap(block, axis, bit):
    count = lax.axis_size(axis)
    return lax.ppermute(block, axis, [(i, i ^ bit) for i in range(count)])


def pick(block, dim, which):
    return lax.squeeze(lax.dynamic_slice_in_dim(block, which, 1, dim), (dim,))


def reduce_whole(block, axis):
    count = lax.axis_size(axis)
    if count < 2 or count & (count - 1):
        return lax.psum(block, axis)
    core = lax.axis_index(axis) & 1
    halves = block.reshape((2, block.shape[0] // 2) + block.shape[1:])
    mine = pick(halves, 0, core) + bit_swap(pick(halves, 0, 1 - core), axis, 1)
    bit = 2
    while bit < count:
        mine = mine + bit_swap(mine, axis, bit)
        bit *= 2
    other = bit_swap(mine, axis, 1)
    low = jnp.where(core == 0, mine, other)
    high = jnp.where(core == 0, other, mine)
    return jnp.concatenate([low, high], axis=0)


def reduce_owned(block, axis):
    count = lax.axis_size(axis)
    if count & (count - 1):
        return lax.psum_scatter(block, axis, scatter_dimension=0, tiled=True)
    me = lax.axis_index(axis)
    owned = block.shape[0] // count
    block = block.reshape((count, owned) + block.shape[1:])
    bit = 1
    while bit < count:
        side = (me // bit) & 1
        pairs = block.reshape((block.shape[0] // 2, 2) + block.shape[1:])
        block = pick(pairs, 1, side) + bit_swap(pick(pairs, 1, 1 - side), axis, bit)
        bit *= 2
    return block.reshape(block.shape[1:])


def observe_block(whole_cols, indices, live, background, targets, weights, w_in, b_in, w_out):
    sampled = jnp.take(whole_cols, indices, axis=0)
    inputs = (background.astype(jnp.float32) + sampled).astype(jnp.bfloat16)
    hidden_pre = jnp.dot(inputs, w_in, preferred_element_type=jnp.float32) + b_in
    hidden, pullback = jax.vjp(gelu_tanh, hidden_pre)
    hidden_low = hidden.astype(jnp.bfloat16)
    outputs = jnp.dot(hidden_low, w_out, preferred_element_type=jnp.float32)
    misfit = ((outputs - targets.astype(jnp.float32)) * (weights * live)[:, None]).astype(
        jnp.bfloat16
    )
    back_hidden = lax.dot_general(
        misfit, w_out, (((1,), (1,)), ((), ())), preferred_element_type=jnp.float32
    )
    (back_pre,) = pullback(back_hidden)
    back_pre = back_pre.astype(jnp.bfloat16)
    back_input = lax.dot_general(
        back_pre, w_in, (((1,), (1,)), ((), ())), preferred_element_type=jnp.float32
    )
    back_input = back_input.astype(jnp.bfloat16)
    column_ids = lax.broadcasted_iota(jnp.int32, (indices.shape[0], whole_cols.shape[0]), 1)
    one_hot = (indices[:, None] == column_ids).astype(jnp.bfloat16)
    return lax.dot_general(
        one_hot, back_input, (((0,), (0,)), ((), ())), preferred_element_type=jnp.float32
    )


def per_device(
    control,
    perturb,
    obs_column,
    obs_count,
    obs_background,
    obs_value,
    obs_weight,
    w_in,
    b_in,
    w_out,
):
    field = control.astype(jnp.float32)
    padded = padded_2(field, (("sub", 1),), SWEEPS)
    for sweep_index in range(SWEEPS):
        padded = sweep(padded)
    field = padded
    partial_sum = jnp.sum(field * perturb.astype(jnp.float32), axis=0)
    members = perturb.shape[0] * lax.axis_size("mem")
    scale = (members - 1) ** (-0.5)
    owned = partial_sum.shape[0] // lax.axis_size("mem")
    whole_cols = reduce_whole(partial_sum, "mem") * scale
    increment = lax.dynamic_slice_in_dim(whole_cols, lax.axis_index("mem") * owned, owned, 0)
    indices = obs_column.reshape(-1)
    background = obs_background.reshape(indices.shape[0], -1)
    targets = obs_value.reshape(indices.shape[0], -1)
    weights = obs_weight.reshape(-1)
    live_count = obs_count.reshape(())
    slot_ids = lax.broadcasted_iota(jnp.int32, (indices.shape[0],), 0)
    live = (slot_ids < live_count).astype(jnp.float32)
    gradient = observe_block(
        whole_cols, indices, live, background, targets, weights, w_in, b_in, w_out
    )
    grad_columns = reduce_owned(gradient, "mem")
    return (increment, grad_columns)


def solution(mesh):
    return jax.shard_map(
        per_device,
        mesh=mesh,
        in_specs=(
            P("mem", "sub", None),
            P("mem", "sub", None),
            P("mem", "sub", None),
            P("mem", "sub"),
            P("mem", "sub", None, None),
            P("mem", "sub", None, None),
            P("mem", "sub", None),
            P(),
            P(),
            P(),
        ),
        out_specs=(P(("sub", "mem"), None), P(("sub", "mem"), None)),
        check_vma=False,
    )
```

```python
import functools

import jax
import jax.numpy as jnp
from jax import lax
from jax.experimental import pallas as pl
from jax.experimental.pallas import tpu as pltpu
from jax.sharding import PartitionSpec as P

SWEEPS = 4


diffusion = 0.4
GELU_ROOT = 0.7978845608028654
GELU_CUBE = 0.044715

def padded_2(block, sides, width):
    for axis, dim in sides:
        count = lax.axis_size(axis)
        forward = [(i, i + 1) for i in range(count - 1)]
        forward.append((count - 1, 0))
        backward = [(target, source) for source, target in forward]
        low = lax.ppermute(
            lax.slice_in_dim(block, block.shape[dim] - width, None, axis=dim), axis, forward
        )
        high = lax.ppermute(lax.slice_in_dim(block, 0, width, axis=dim), axis, backward)
        block = jnp.concatenate([low, block, high], axis=dim)
    return block


def sweep(padded):
    middle = padded[:, 1:-1]
    return middle + diffusion * (padded[:, :-2] - 2.0 * middle + padded[:, 2:])


def pair_swap(block, axis, low_bit, high_bit):
    count = lax.axis_size(axis)
    pairs = [(i, i ^ (high_bit if i & 1 else low_bit)) for i in range(count)]
    return lax.ppermute(block, axis, pairs)


def pick(block, dim, which):
    return lax.squeeze(lax.dynamic_slice_in_dim(block, which, 1, dim), (dim,))


def chip_bits(count):
    return [1 << step for step in range(1, count.bit_length() - 1)]


def reduce_pairs(block, axis):
    count = lax.axis_size(axis)
    core = lax.axis_index(axis) & 1
    sides = block.reshape((count // 2, 2, block.shape[0] // count) + block.shape[1:])
    mine = pick(sides, 1, core) + pair_swap(pick(sides, 1, 1 - core), axis, 1, 1)
    bits = chip_bits(count)
    for low_bit, high_bit in zip(bits, bits[::-1]):
        mine = mine + pair_swap(mine, axis, low_bit, high_bit)
    mine = mine.reshape((-1,) + block.shape[1:])
    return mine, pair_swap(mine, axis, 1, 1)


def scatter_pairs(keep, send, axis):
    count = lax.axis_size(axis)
    me = lax.axis_index(axis)
    block = keep + pair_swap(send, axis, 1, 1)
    for bit in chip_bits(count):
        side = (me // bit) & 1
        halves = block.reshape((-1, 2) + keep.shape[1:])
        block = pick(halves, 1, side) + pair_swap(pick(halves, 1, 1 - side), axis, bit, bit)
    return block.reshape(keep.shape[1:])


def observe_kernel(
    mine, other, indices, weights, background, targets, w_in, b_in, w_out, keep, send, slope, *, scale, block, chunk
):
    slots, levels = background.shape
    half_columns = mine.shape[0]
    columns = 2 * half_columns
    hidden = w_in.shape[1]
    increment = jnp.concatenate([mine[...], other[...]], axis=0) * scale
    top = increment.astype(jnp.bfloat16)
    rest = (increment - top.astype(jnp.float32)).astype(jnp.bfloat16)
    table = jnp.concatenate([top, rest], axis=1)

    def start(index):
        base = index * block
        row = indices[0:1, base:base + block]
        across = lax.broadcasted_iota(jnp.int32, (columns, block), 0) == row
        picked = across.astype(jnp.float32).astype(jnp.bfloat16)
        pair = lax.dot_general(picked, table, (((0,), (0,)), ((), ())), preferred_element_type=jnp.float32)
        sampled = pair[:, :levels] + pair[:, levels:]
        inputs = (background[base:base + block, :].astype(jnp.float32) + sampled).astype(jnp.bfloat16)
        return dict(base=base, slot=index % 2, picked=picked, inputs=inputs, outputs=None, back=None)

    def forward(st, c):
        sl = slice(c, c + chunk)
        pre = jnp.dot(st["inputs"], w_in[:, sl], preferred_element_type=jnp.float32) + b_in[0:1, sl]
        square = pre * pre
        bend = jnp.tanh(pre * (GELU_ROOT + GELU_ROOT * GELU_CUBE * square))
        half = 0.5 * pre
        lift = 1.0 + bend
        st_hidden = (half * lift).astype(jnp.bfloat16)
        rise = GELU_ROOT + 3.0 * GELU_ROOT * GELU_CUBE * square
        tilt = lift * (0.5 + half * ((1.0 - bend) * rise))
        slope[st["slot"], :, sl] = tilt
        part = jnp.dot(st_hidden, w_out[sl, :], preferred_element_type=jnp.float32)
        st["outputs"] = part if st["outputs"] is None else st["outputs"] + part

    def middle(st):
        base = st["base"]
        row = weights[0:1, base:base + block]
        col = jnp.transpose(jnp.broadcast_to(row, (targets.shape[1], block)))
        st["misfit"] = ((st["outputs"] - targets[base:base + block, :].astype(jnp.float32)) * col).astype(jnp.bfloat16)

    def backward(st, c):
        sl = slice(c, c + chunk)
        back = lax.dot_general(st["misfit"], w_out[sl, :], (((1,), (1,)), ((), ())), preferred_element_type=jnp.float32)
        back = (back * slope[st["slot"], :, sl]).astype(jnp.bfloat16)
        part = lax.dot_general(back, w_in[:, sl], (((1,), (1,)), ((), ())), preferred_element_type=jnp.float32)
        st["back"] = part if st["back"] is None else st["back"] + part

    def finish(st, total):
        part = jnp.dot(st["picked"], st["back"].astype(jnp.bfloat16), preferred_element_type=jnp.float32)
        return part if total is None else total + part

    blocks = slots // block
    total = None
    behind = None
    for index in range(blocks + 1):
        ahead = start(index) if index < blocks else None
        for c in range(0, hidden, chunk):
            if ahead is not None:
                forward(ahead, c)
            if behind is not None:
                backward(behind, c)
        if behind is not None:
            total = finish(behind, total)
        if ahead is not None:
            middle(ahead)
        behind = ahead
    keep[...] = total[:half_columns]
    send[...] = total[half_columns:]


def largest_part(size, limit):
    part = min(size, limit)
    while size % part:
        part -= 1
    return part


def observe_call(mine, other, indices, weights, background, targets, w_in, b_in, w_out, scale):
    vm = pl.BlockSpec(memory_space=pltpu.VMEM)
    block = largest_part(background.shape[0], 512)
    chunk = largest_part(w_in.shape[1], 256)
    half = jax.ShapeDtypeStruct(mine.shape, jnp.float32)
    return pl.pallas_call(
        functools.partial(observe_kernel, scale=scale, block=block, chunk=chunk),
        out_shape=(half, half),
        in_specs=[vm] * 9,
        out_specs=(vm, vm),
        scratch_shapes=[pltpu.VMEM((2, block, w_in.shape[1]), jnp.float32)],
        name="observe",
    )(mine, other, indices, weights, background, targets, w_in, b_in, w_out)


def per_device(
    control,
    perturb,
    obs_column,
    obs_count,
    obs_background,
    obs_value,
    obs_weight,
    w_in,
    b_in,
    w_out,
):
    field = control.astype(jnp.float32)
    padded = padded_2(field, (("sub", 1),), SWEEPS)
    for sweep_index in range(SWEEPS):
        padded = sweep(padded)
    field = padded
    partial_sum = jnp.sum(field * perturb.astype(jnp.float32), axis=0)
    members = perturb.shape[0] * lax.axis_size("mem")
    scale = (members - 1) ** (-0.5)
    count = lax.axis_size("mem")
    me = lax.axis_index("mem")
    columns = partial_sum.shape[0]
    owned = columns // count
    indices = obs_column.reshape(1, -1)
    slots = indices.shape[1]
    paired = count > 1 and count & (count - 1) == 0
    if paired:
        owner = indices // owned
        side = ((owner ^ me) & 1) * (columns // 2)
        indices = side + (owner // 2) * owned + indices % owned
        mine, other = reduce_pairs(partial_sum, "mem")
        increment = pick(mine.reshape(count // 2, owned, -1), 0, me // 2) * scale
    else:
        summed = lax.psum(partial_sum, "mem")
        mine, other = summed[: columns // 2], summed[columns // 2 :]
        increment = lax.dynamic_slice_in_dim(summed, me * owned, owned, 0) * scale
    slot_ids = lax.broadcasted_iota(jnp.int32, (1, slots), 1)
    live = (slot_ids < obs_count.reshape(())).astype(jnp.float32)
    keep, send = observe_call(
        mine,
        other,
        indices,
        obs_weight.reshape(1, slots) * live,
        obs_background.reshape(slots, -1),
        obs_value.reshape(slots, -1),
        w_in,
        b_in.reshape(1, -1),
        w_out,
        scale,
    )
    if paired:
        halves = (count // 2, owned, keep.shape[1])
        grad_columns = scatter_pairs(keep.reshape(halves), send.reshape(halves), "mem")
    else:
        gradient = jnp.concatenate([keep, send], axis=0)
        grad_columns = lax.psum_scatter(gradient, "mem", scatter_dimension=0, tiled=True)
    return (increment, grad_columns)


def solution(mesh):
    return jax.shard_map(
        per_device,
        mesh=mesh,
        in_specs=(
            P("mem", "sub", None),
            P("mem", "sub", None),
            P("mem", "sub", None),
            P("mem", "sub"),
            P("mem", "sub", None, None),
            P("mem", "sub", None, None),
            P("mem", "sub", None),
            P(),
            P(),
            P(),
        ),
        out_specs=(P(("sub", "mem"), None), P(("sub", "mem"), None)),
        check_vma=False,
    )
```

```python
import functools

import jax
import jax.numpy as jnp
from jax import lax
from jax.experimental import pallas as pl
from jax.experimental.pallas import tpu as pltpu
from jax.sharding import PartitionSpec as P

SWEEPS = 4


diffusion = 0.4
GELU_ROOT = 0.7978845608028654
GELU_CUBE = 0.044715

ON_CHIP = pl.BlockSpec(memory_space=pltpu.VMEM)
EDGE = 8 * -(-SWEEPS // 8)


def near(*arrays):
    return [pltpu.with_memory_space_constraint(a, pltpu.VMEM) for a in arrays]


def edge_columns(block, axis):
    count = lax.axis_size(axis)
    forward = [(i, (i + 1) % count) for i in range(count)]
    backward = [(target, source) for source, target in forward]
    first = block[:, :EDGE].astype(jnp.float32)
    last = block[:, -EDGE:].astype(jnp.float32)
    return lax.ppermute(last, axis, forward), lax.ppermute(first, axis, backward)


def swept(field):
    rows = field.shape[0]
    for sweep_index in range(SWEEPS):
        low = pltpu.roll(field, 1, 0)
        high = pltpu.roll(field, rows - 1, 0)
        field = field + diffusion * ((low - 2.0 * field) + high)
    return field


def inside_kernel(control, perturb, total, ends, factors):
    members, columns, levels = control.shape
    summed = None
    for member in range(members):
        field = control[member].astype(jnp.float32)
        factor = perturb[member].astype(jnp.float32)
        ends[member, :EDGE] = field[:EDGE]
        ends[member, EDGE:] = field[columns - EDGE:]
        factors[member, :EDGE] = factor[:EDGE]
        factors[member, EDGE:] = factor[columns - EDGE:]
        part = swept(field) * factor
        summed = part if summed is None else summed + part
    total[...] = summed


def edge_kernel(core, inside, ends, factors, low, high, keep, send, total, *, owners):
    members = ends.shape[0]
    columns, levels = total.shape
    total[...] = inside[...]
    windows = []
    for member in range(members):
        windows += [low[member], ends[member], high[member]]
    field = swept(jnp.concatenate(windows, axis=0))
    size = 4 * EDGE
    start = jnp.zeros((EDGE, levels), jnp.float32)
    stop = start
    for member in range(members):
        base = size * member + EDGE
        start = start + field[base:base + EDGE] * factors[member, :EDGE]
        stop = stop + field[base + EDGE:base + 2 * EDGE] * factors[member, EDGE:]
    rows = lax.broadcasted_iota(jnp.int32, (EDGE, levels), 0)
    total[:EDGE] = jnp.where(rows < SWEEPS, start, total[:EDGE])
    total[columns - EDGE:] = jnp.where(rows >= EDGE - SWEEPS, stop, total[columns - EDGE:])
    owned = columns // owners
    for chip in range(owners // 2):
        here = pl.multiple_of((2 * chip + core[0]) * owned, owned)
        there = pl.multiple_of((2 * chip + 1 - core[0]) * owned, owned)
        keep[chip * owned:(chip + 1) * owned] = total[pl.ds(here, owned)]
        send[chip * owned:(chip + 1) * owned] = total[pl.ds(there, owned)]


def member_sum(control, perturb, core, owners):
    members, columns, levels = control.shape
    low, high = edge_columns(control, "sub")
    ends = pltpu.VMEM((members, 2 * EDGE, levels), jnp.float32)
    whole = pltpu.VMEM((columns, levels), jnp.float32)
    total, fields, factors = pl.pallas_call(
        inside_kernel,
        out_shape=(whole, ends, ends),
        in_specs=[ON_CHIP] * 2,
        out_specs=(ON_CHIP,) * 3,
        name="inside",
    )(control, perturb)
    half = pltpu.VMEM((columns // 2, levels), jnp.float32)
    return pl.pallas_call(
        functools.partial(edge_kernel, owners=owners),
        out_shape=(half, half),
        in_specs=[pl.BlockSpec(memory_space=pltpu.SMEM)] + [ON_CHIP] * 5,
        out_specs=(ON_CHIP,) * 2,
        scratch_shapes=[whole],
        name="edges",
    )(core, *near(total, fields, factors, low, high))


def bit_swap(block, axis, bit):
    count = lax.axis_size(axis)
    return lax.ppermute(block, axis, [(i, i ^ bit) for i in range(count)])


def pick(block, dim, which):
    return lax.squeeze(lax.dynamic_slice_in_dim(block, which, 1, dim), (dim,))


def reduce_pairs(keep, send, axis):
    count = lax.axis_size(axis)
    mine = keep + bit_swap(send, axis, 1)
    if count <= 8:
        parts = [bit_swap(mine, axis, bit) for bit in range(2, count, 2)]
        for part in parts:
            mine = mine + part
    else:
        for step in range(1, count.bit_length() - 1):
            mine = mine + bit_swap(mine, axis, 1 << step)
    return mine, bit_swap(mine, axis, 1)


def scatter_pairs(keep, send, axis):
    count = lax.axis_size(axis)
    me = lax.axis_index(axis)
    block = keep + bit_swap(send, axis, 1)
    block = block.reshape((count // 2, -1) + block.shape[1:])
    for step in range(1, count.bit_length() - 1):
        side = (me >> step) & 1
        halves = block.reshape((-1, 2) + block.shape[1:])
        block = pick(halves, 1, side) + bit_swap(pick(halves, 1, 1 - side), axis, 1 << step)
    return block.reshape(block.shape[1:])


def observe_kernel(
    mine, other, indices, weights, background, targets, w_in, b_in, w_out, keep, send, slope, *, scale, block, chunk
):
    slots, levels = background.shape
    half_columns = mine.shape[0]
    columns = 2 * half_columns
    hidden = w_in.shape[1]
    increment = jnp.concatenate([mine[...], other[...]], axis=0) * scale
    top = increment.astype(jnp.bfloat16)
    rest = (increment - top.astype(jnp.float32)).astype(jnp.bfloat16)
    table = jnp.concatenate([top, rest], axis=1)
    half_bias = 0.5 * b_in[...]

    def start(index):
        base = index * block
        row = indices[0:1, base:base + block]
        across = lax.broadcasted_iota(jnp.int32, (columns, block), 0) == row
        picked = across.astype(jnp.float32).astype(jnp.bfloat16)
        pair = lax.dot_general(picked, table, (((0,), (0,)), ((), ())), preferred_element_type=jnp.float32)
        sampled = pair[:, :levels] + pair[:, levels:]
        inputs = 0.5 * (background[base:base + block, :].astype(jnp.float32) + sampled).astype(jnp.bfloat16)
        return dict(base=base, slot=index % 2, picked=picked, inputs=inputs, outputs=None, back=None)

    def forward(st, c):
        sl = slice(c, c + chunk)
        half = jnp.dot(st["inputs"], w_in[:, sl], preferred_element_type=jnp.float32) + half_bias[0:1, sl]
        square = half * half
        bend = jnp.tanh(half * (2.0 * GELU_ROOT + 8.0 * GELU_ROOT * GELU_CUBE * square))
        lift = 1.0 + bend
        st_hidden = (half * lift).astype(jnp.bfloat16)
        rise = GELU_ROOT + 12.0 * GELU_ROOT * GELU_CUBE * square
        tilt = lift * (0.5 + half * ((1.0 - bend) * rise))
        slope[st["slot"], :, sl] = tilt
        part = jnp.dot(st_hidden, w_out[sl, :], preferred_element_type=jnp.float32)
        st["outputs"] = part if st["outputs"] is None else st["outputs"] + part

    def middle(st):
        base = st["base"]
        row = weights[0:1, base:base + block]
        col = jnp.transpose(jnp.broadcast_to(row, (targets.shape[1], block)))
        st["misfit"] = ((st["outputs"] - targets[base:base + block, :].astype(jnp.float32)) * col).astype(jnp.bfloat16)

    def backward(st, c):
        sl = slice(c, c + chunk)
        back = lax.dot_general(st["misfit"], w_out[sl, :], (((1,), (1,)), ((), ())), preferred_element_type=jnp.float32)
        back = (back * slope[st["slot"], :, sl]).astype(jnp.bfloat16)
        part = lax.dot_general(back, w_in[:, sl], (((1,), (1,)), ((), ())), preferred_element_type=jnp.float32)
        st["back"] = part if st["back"] is None else st["back"] + part

    def finish(st, total):
        part = jnp.dot(st["picked"], st["back"].astype(jnp.bfloat16), preferred_element_type=jnp.float32)
        return part if total is None else total + part

    blocks = slots // block
    total = None
    behind = None
    for index in range(blocks + 1):
        ahead = start(index) if index < blocks else None
        for c in range(0, hidden, chunk):
            if ahead is not None:
                forward(ahead, c)
            if behind is not None:
                backward(behind, c)
        if behind is not None:
            total = finish(behind, total)
        if ahead is not None:
            middle(ahead)
        behind = ahead
    keep[...] = total[:half_columns]
    send[...] = total[half_columns:]


def largest_part(size, limit):
    part = min(size, limit)
    while size % part:
        part -= 1
    return part


def observe_call(mine, other, indices, weights, background, targets, w_in, b_in, w_out, scale):
    block = largest_part(background.shape[0], 512)
    chunk = largest_part(w_in.shape[1], 256)
    half = pltpu.VMEM(mine.shape, jnp.float32)
    return pl.pallas_call(
        functools.partial(observe_kernel, scale=scale, block=block, chunk=chunk),
        out_shape=(half, half),
        in_specs=[ON_CHIP] * 9,
        out_specs=(ON_CHIP, ON_CHIP),
        scratch_shapes=[pltpu.VMEM((2, block, w_in.shape[1]), jnp.float32)],
        name="observe",
    )(*near(mine, other, indices, weights, background, targets, w_in, b_in, w_out))


def per_device(
    control,
    perturb,
    obs_column,
    obs_count,
    obs_background,
    obs_value,
    obs_weight,
    w_in,
    b_in,
    w_out,
):
    members = perturb.shape[0] * lax.axis_size("mem")
    scale = (members - 1) ** (-0.5)
    count = lax.axis_size("mem")
    me = lax.axis_index("mem")
    columns = control.shape[1]
    owned = columns // count
    indices = obs_column.reshape(1, -1)
    slots = indices.shape[1]
    paired = count > 1 and count & (count - 1) == 0
    core = me & 1 if paired else jnp.int32(0)
    keep, send = member_sum(control, perturb, core.reshape(1), count if paired else 2)
    if paired:
        owner = indices // owned
        side = ((owner ^ me) & 1) * (columns // 2)
        indices = side + (owner // 2) * owned + indices % owned
        mine, other = reduce_pairs(keep, send, "mem")
        increment = pick(mine.reshape(count // 2, owned, -1), 0, me // 2) * scale
    else:
        summed = lax.psum(jnp.concatenate([keep, send], axis=0), "mem")
        mine, other = summed[: columns // 2], summed[columns // 2 :]
        increment = lax.dynamic_slice_in_dim(summed, me * owned, owned, 0) * scale
    slot_ids = lax.broadcasted_iota(jnp.int32, (1, slots), 1)
    live = (slot_ids < obs_count.reshape(())).astype(jnp.float32)
    keep, send = observe_call(
        mine,
        other,
        indices,
        obs_weight.reshape(1, slots) * live,
        obs_background.reshape(slots, -1),
        obs_value.reshape(slots, -1),
        w_in,
        b_in.reshape(1, -1),
        w_out,
        scale,
    )
    if paired:
        grad_columns = scatter_pairs(keep, send, "mem")
    else:
        gradient = jnp.concatenate([keep, send], axis=0)
        grad_columns = lax.psum_scatter(gradient, "mem", scatter_dimension=0, tiled=True)
    return (increment, grad_columns)


def solution(mesh):
    return jax.shard_map(
        per_device,
        mesh=mesh,
        in_specs=(
            P("mem", "sub", None),
            P("mem", "sub", None),
            P("mem", "sub", None),
            P("mem", "sub"),
            P("mem", "sub", None, None),
            P("mem", "sub", None, None),
            P("mem", "sub", None),
            P(),
            P(),
            P(),
        ),
        out_specs=(P(("sub", "mem"), None), P(("sub", "mem"), None)),
        check_vma=False,
    )
```

```python
import functools

import jax
import jax.numpy as jnp
from jax import lax
from jax.experimental import pallas as pl
from jax.experimental.pallas import tpu as pltpu
from jax.sharding import PartitionSpec as P

SWEEPS = 4


diffusion = 0.4
GELU_ROOT = 0.7978845608028654
GELU_CUBE = 0.044715

ON_CHIP = pl.BlockSpec(memory_space=pltpu.VMEM)
EDGE = 8 * -(-SWEEPS // 8)


def near(*arrays):
    return [pltpu.with_memory_space_constraint(a, pltpu.VMEM) for a in arrays]


def room(mebibytes):
    return pltpu.CompilerParams(vmem_limit_bytes=mebibytes << 20)


def edge_columns(block, axis):
    count = lax.axis_size(axis)
    forward = [(i, (i + 1) % count) for i in range(count)]
    backward = [(target, source) for source, target in forward]
    first = block[:, :EDGE].astype(jnp.float32)
    last = block[:, -EDGE:].astype(jnp.float32)
    return lax.ppermute(last, axis, forward), lax.ppermute(first, axis, backward)


def swept(field):
    rows = field.shape[0]
    for sweep_index in range(SWEEPS):
        low = pltpu.roll(field, 1, 0)
        high = pltpu.roll(field, rows - 1, 0)
        field = field + diffusion * ((low - 2.0 * field) + high)
    return field


def inside_kernel(control, perturb, total, ends, factors, fields, weights, arrived):
    members, columns, levels = control.shape
    copies = []
    for member in range(members):
        copies.append((
            pltpu.make_async_copy(control.at[member], fields.at[member], arrived.at[0, member]),
            pltpu.make_async_copy(perturb.at[member], weights.at[member], arrived.at[1, member]),
        ))
    for pair in copies:
        for copy in pair:
            copy.start()
    summed = None
    for member in range(members):
        for copy in copies[member]:
            copy.wait()
        field = fields[member].astype(jnp.float32)
        factor = weights[member].astype(jnp.float32)
        ends[member, :EDGE] = field[:EDGE]
        ends[member, EDGE:] = field[columns - EDGE:]
        factors[member, :EDGE] = factor[:EDGE]
        factors[member, EDGE:] = factor[columns - EDGE:]
        part = swept(field) * factor
        summed = part if summed is None else summed + part
    total[...] = summed


def edge_kernel(core, inside, ends, factors, low, high, keep, send, total, *, owners):
    members = ends.shape[0]
    columns, levels = total.shape
    total[...] = inside[...]
    windows = []
    for member in range(members):
        windows += [low[member], ends[member], high[member]]
    field = swept(jnp.concatenate(windows, axis=0))
    size = 4 * EDGE
    start = jnp.zeros((EDGE, levels), jnp.float32)
    stop = start
    for member in range(members):
        base = size * member + EDGE
        start = start + field[base:base + EDGE] * factors[member, :EDGE]
        stop = stop + field[base + EDGE:base + 2 * EDGE] * factors[member, EDGE:]
    rows = lax.broadcasted_iota(jnp.int32, (EDGE, levels), 0)
    total[:EDGE] = jnp.where(rows < SWEEPS, start, total[:EDGE])
    total[columns - EDGE:] = jnp.where(rows >= EDGE - SWEEPS, stop, total[columns - EDGE:])
    owned = columns // owners
    for chip in range(owners // 2):
        here = pl.multiple_of((2 * chip + core[0]) * owned, owned)
        there = pl.multiple_of((2 * chip + 1 - core[0]) * owned, owned)
        keep[chip * owned:(chip + 1) * owned] = total[pl.ds(here, owned)]
        send[chip * owned:(chip + 1) * owned] = total[pl.ds(there, owned)]


def member_sum(control, perturb, core, owners):
    members, columns, levels = control.shape
    low, high = edge_columns(control, "sub")
    ends = pltpu.VMEM((members, 2 * EDGE, levels), jnp.float32)
    whole = pltpu.VMEM((columns, levels), jnp.float32)
    total, fields, factors = pl.pallas_call(
        inside_kernel,
        out_shape=(whole, ends, ends),
        in_specs=[pl.BlockSpec(memory_space=pltpu.HBM)] * 2,
        out_specs=(ON_CHIP,) * 3,
        scratch_shapes=[
            pltpu.VMEM(control.shape, control.dtype),
            pltpu.VMEM(perturb.shape, perturb.dtype),
            pltpu.SemaphoreType.DMA((2, members)),
        ],
        compiler_params=room(16),
        name="inside",
    )(*(pltpu.with_memory_space_constraint(a, pltpu.HBM) for a in (control, perturb)))
    half = pltpu.VMEM((columns // 2, levels), jnp.float32)
    return pl.pallas_call(
        functools.partial(edge_kernel, owners=owners),
        out_shape=(half, half),
        in_specs=[pl.BlockSpec(memory_space=pltpu.SMEM)] + [ON_CHIP] * 5,
        out_specs=(ON_CHIP,) * 2,
        scratch_shapes=[whole],
        compiler_params=room(16),
        name="edges",
    )(core, *near(total, fields, factors, low, high))


def bit_swap(block, axis, bit):
    count = lax.axis_size(axis)
    return lax.ppermute(block, axis, [(i, i ^ bit) for i in range(count)])


def pick(block, dim, which):
    return lax.squeeze(lax.dynamic_slice_in_dim(block, which, 1, dim), (dim,))


def reduce_pairs(keep, send, axis):
    count = lax.axis_size(axis)
    mine = keep + bit_swap(send, axis, 1)
    if count <= 8:
        parts = [bit_swap(mine, axis, bit) for bit in range(2, count, 2)]
        for part in parts:
            mine = mine + part
    else:
        for step in range(1, count.bit_length() - 1):
            mine = mine + bit_swap(mine, axis, 1 << step)
    return mine, bit_swap(mine, axis, 1)


def scatter_pairs(keep, send, axis):
    count = lax.axis_size(axis)
    me = lax.axis_index(axis)
    block = keep + bit_swap(send, axis, 1)
    block = block.reshape((count // 2, -1) + block.shape[1:])
    if count <= 8:
        chip = me >> 1
        bits = list(range(1, count // 2))
        parts = [bit_swap(pick(block, 0, chip ^ bit), axis, 2 * bit) for bit in bits[-1:] + bits[:-1]]
        owned = pick(block, 0, chip)
        for part in parts:
            owned = owned + part
        return owned
    for step in range(1, count.bit_length() - 1):
        side = (me >> step) & 1
        halves = block.reshape((-1, 2) + block.shape[1:])
        block = pick(halves, 1, side) + bit_swap(pick(halves, 1, 1 - side), axis, 1 << step)
    return block.reshape(block.shape[1:])


def layout_kernel(count, indices, weights, by_column, by_slot, spread):
    columns, slots = by_column.shape
    lanes = spread.shape[1]
    row = indices[...]
    picked = (lax.broadcasted_iota(jnp.int32, (columns, slots), 0) == row).astype(jnp.float32)
    by_column[...] = picked.astype(jnp.bfloat16)
    by_slot[...] = jnp.transpose(picked).astype(jnp.bfloat16)
    live = lax.broadcasted_iota(jnp.int32, (1, slots), 1) < count[0, 0]
    spread[...] = jnp.transpose(jnp.broadcast_to(jnp.where(live, weights[...], 0.0), (lanes, slots)))


def layout_call(count, indices, weights, columns, lanes):
    slots = indices.shape[1]
    return pl.pallas_call(
        layout_kernel,
        out_shape=(
            pltpu.VMEM((columns, slots), jnp.bfloat16),
            pltpu.VMEM((slots, columns), jnp.bfloat16),
            pltpu.VMEM((slots, lanes), jnp.float32),
        ),
        in_specs=[pl.BlockSpec(memory_space=pltpu.SMEM)] + [ON_CHIP] * 2,
        out_specs=(ON_CHIP,) * 3,
        compiler_params=room(16),
        name="layout",
    )(count, *near(indices, weights))


def observe_kernel(
    mine, other, by_column, by_slot, spread, background, targets, w_in, b_in, w_out, keep, send, slope, *, scale, block, chunk
):
    slots, levels = background.shape
    half_columns = mine.shape[0]
    hidden = w_in.shape[1]
    increment = jnp.concatenate([mine[...], other[...]], axis=0) * scale
    top = increment.astype(jnp.bfloat16)
    rest = (increment - top.astype(jnp.float32)).astype(jnp.bfloat16)
    table = jnp.concatenate([top, rest], axis=1)
    half_bias = 0.5 * b_in[...]

    def start(index):
        base = index * block
        pair = jnp.dot(by_slot[base:base + block, :], table, preferred_element_type=jnp.float32)
        sampled = pair[:, :levels] + pair[:, levels:]
        inputs = 0.5 * (background[base:base + block, :].astype(jnp.float32) + sampled).astype(jnp.bfloat16)
        return dict(base=base, slot=index % 2, inputs=inputs, outputs=None, back=None)

    def forward(st, c):
        sl = slice(c, c + chunk)
        half = jnp.dot(st["inputs"], w_in[:, sl], preferred_element_type=jnp.float32) + half_bias[0:1, sl]
        square = half * half
        bend = jnp.tanh(half * (2.0 * GELU_ROOT + 8.0 * GELU_ROOT * GELU_CUBE * square))
        lift = 1.0 + bend
        st_hidden = (half * lift).astype(jnp.bfloat16)
        rise = GELU_ROOT + 12.0 * GELU_ROOT * GELU_CUBE * square
        tilt = lift * (0.5 + half * ((1.0 - bend) * rise))
        slope[st["slot"], :, sl] = tilt
        part = jnp.dot(st_hidden, w_out[sl, :], preferred_element_type=jnp.float32)
        st["outputs"] = part if st["outputs"] is None else st["outputs"] + part

    def middle(st):
        base = st["base"]
        col = spread[base:base + block, :]
        st["misfit"] = ((st["outputs"] - targets[base:base + block, :].astype(jnp.float32)) * col).astype(jnp.bfloat16)

    def backward(st, c):
        sl = slice(c, c + chunk)
        back = lax.dot_general(st["misfit"], w_out[sl, :], (((1,), (1,)), ((), ())), preferred_element_type=jnp.float32)
        back = (back * slope[st["slot"], :, sl]).astype(jnp.bfloat16)
        part = lax.dot_general(back, w_in[:, sl], (((1,), (1,)), ((), ())), preferred_element_type=jnp.float32)
        st["back"] = part if st["back"] is None else st["back"] + part

    def finish(st, total):
        picked = by_column[:, st["base"]:st["base"] + block]
        part = jnp.dot(picked, st["back"].astype(jnp.bfloat16), preferred_element_type=jnp.float32)
        return part if total is None else total + part

    blocks = slots // block
    total = None
    behind = None
    for index in range(blocks + 1):
        ahead = start(index) if index < blocks else None
        for c in range(0, hidden, chunk):
            if ahead is not None:
                forward(ahead, c)
            if behind is not None:
                backward(behind, c)
        if behind is not None:
            total = finish(behind, total)
        if ahead is not None:
            middle(ahead)
        behind = ahead
    keep[...] = total[:half_columns]
    send[...] = total[half_columns:]


def largest_part(size, limit):
    part = min(size, limit)
    while size % part:
        part -= 1
    return part


def observe_call(mine, other, by_column, by_slot, spread, background, targets, w_in, b_in, w_out, scale):
    block = largest_part(background.shape[0], 512)
    chunk = largest_part(w_in.shape[1], 256)
    half = pltpu.VMEM(mine.shape, jnp.float32)
    return pl.pallas_call(
        functools.partial(observe_kernel, scale=scale, block=block, chunk=chunk),
        out_shape=(half, half),
        in_specs=[ON_CHIP] * 10,
        out_specs=(ON_CHIP, ON_CHIP),
        scratch_shapes=[pltpu.VMEM((2, block, w_in.shape[1]), jnp.float32)],
        compiler_params=room(32),
        name="observe",
    )(*near(mine, other, by_column, by_slot, spread, background, targets, w_in, b_in, w_out))


def per_device(
    control,
    perturb,
    obs_column,
    obs_count,
    obs_background,
    obs_value,
    obs_weight,
    w_in,
    b_in,
    w_out,
):
    members = perturb.shape[0] * lax.axis_size("mem")
    scale = (members - 1) ** (-0.5)
    count = lax.axis_size("mem")
    me = lax.axis_index("mem")
    columns = control.shape[1]
    owned = columns // count
    indices = obs_column.reshape(1, -1)
    slots = indices.shape[1]
    paired = count > 1 and count & (count - 1) == 0
    core = me & 1 if paired else jnp.int32(0)
    keep, send = member_sum(control, perturb, core.reshape(1), count if paired else 2)
    if paired:
        owner = indices // owned
        side = ((owner ^ me) & 1) * (columns // 2)
        indices = side + (owner // 2) * owned + indices % owned
        mine, other = reduce_pairs(keep, send, "mem")
        increment = pick(mine.reshape(count // 2, owned, -1), 0, me // 2) * scale
    else:
        summed = lax.psum(jnp.concatenate([keep, send], axis=0), "mem")
        mine, other = summed[: columns // 2], summed[columns // 2 :]
        increment = lax.dynamic_slice_in_dim(summed, me * owned, owned, 0) * scale
    layouts = layout_call(obs_count, indices, obs_weight.reshape(1, slots), columns, obs_value.shape[-1])
    keep, send = observe_call(
        mine,
        other,
        *layouts,
        obs_background.reshape(slots, -1),
        obs_value.reshape(slots, -1),
        w_in,
        b_in.reshape(1, -1),
        w_out,
        scale,
    )
    if paired:
        grad_columns = scatter_pairs(keep, send, "mem")
    else:
        gradient = jnp.concatenate([keep, send], axis=0)
        grad_columns = lax.psum_scatter(gradient, "mem", scatter_dimension=0, tiled=True)
    return (increment, grad_columns)


def solution(mesh):
    return jax.shard_map(
        per_device,
        mesh=mesh,
        in_specs=(
            P("mem", "sub", None),
            P("mem", "sub", None),
            P("mem", "sub", None),
            P("mem", "sub"),
            P("mem", "sub", None, None),
            P("mem", "sub", None, None),
            P("mem", "sub", None),
            P(),
            P(),
            P(),
        ),
        out_specs=(P(("sub", "mem"), None), P(("sub", "mem"), None)),
        check_vma=False,
    )
```

```python
import functools

import jax
import jax.numpy as jnp
from jax import lax
from jax.experimental import pallas as pl
from jax.experimental.pallas import tpu as pltpu
from jax.sharding import PartitionSpec as P

SWEEPS = 4


diffusion = 0.4
GELU_ROOT = 0.7978845608028654
GELU_CUBE = 0.044715

ON_CHIP = pl.BlockSpec(memory_space=pltpu.VMEM)
EDGE = 8 * -(-SWEEPS // 8)


def near(*arrays):
    return [pltpu.with_memory_space_constraint(a, pltpu.VMEM) for a in arrays]


def room(mebibytes):
    return pltpu.CompilerParams(vmem_limit_bytes=mebibytes << 20)


def edge_columns(block, axis):
    count = lax.axis_size(axis)
    forward = [(i, (i + 1) % count) for i in range(count)]
    backward = [(target, source) for source, target in forward]
    first = block[:, :EDGE].astype(jnp.float32)
    last = block[:, -EDGE:].astype(jnp.float32)
    low = lax.ppermute(last, axis, forward)
    high = lax.ppermute(first, axis, backward)
    return low, high


def swept(field):
    rows = field.shape[0]
    for _ in range(SWEEPS):
        low = pltpu.roll(field, 1, 0)
        high = pltpu.roll(field, rows - 1, 0)
        field = field + diffusion * ((low - 2.0 * field) + high)
    return field


def stencil_matrix(columns):
    taps = [1.0]
    for _ in range(SWEEPS):
        wide = [0.0] + taps + [0.0]
        taps = [
            (1.0 - 2.0 * diffusion) * wide[i]
            + diffusion * ((wide[i - 1] if i else 0.0) + (wide[i + 1] if i + 1 < len(wide) else 0.0))
            for i in range(len(wide))
        ]
    row = lax.broadcasted_iota(jnp.int32, (columns, columns), 0)
    apart = jnp.abs(row - lax.broadcasted_iota(jnp.int32, (columns, columns), 1))
    matrix = jnp.zeros((columns, columns), jnp.float32)
    for distance in range(SWEEPS + 1):
        matrix = jnp.where(apart == distance, taps[SWEEPS + distance], matrix)
    top = matrix.astype(jnp.bfloat16)
    return top, (matrix - top.astype(jnp.float32)).astype(jnp.bfloat16)


def inside_kernel(core, control, perturb, keep, send, ends, factors, fields, weights, total, arrived, *, owners):
    members, columns, levels = control.shape
    copies = []
    for member in range(members):
        lanes = slice(member * levels, (member + 1) * levels)
        copies.append((
            pltpu.make_async_copy(control.at[member], fields.at[:, lanes], arrived.at[0, member]),
            pltpu.make_async_copy(perturb.at[member], weights.at[:, lanes], arrived.at[1, member]),
        ))
    for pair in copies:
        for copy in pair:
            copy.start()
    top, rest = stencil_matrix(columns)
    summed = None
    group = 2 if members % 2 == 0 else 1
    for first in range(0, members, group):
        for member in range(first, first + group):
            for copy in copies[member]:
                copy.wait()
        lanes = slice(first * levels, (first + group) * levels)
        field = fields[:, lanes]
        factor = weights[:, lanes].astype(jnp.float32)
        local = jnp.dot(top, field, preferred_element_type=jnp.float32)
        local = local + jnp.dot(rest, field, preferred_element_type=jnp.float32)
        product = local * factor
        for step in range(group):
            here = slice(step * levels, (step + 1) * levels)
            summed = product[:, here] if summed is None else summed + product[:, here]
            member = first + step
            ends[member, :EDGE] = field[:EDGE, here].astype(jnp.float32)
            ends[member, EDGE:] = field[columns - EDGE:, here].astype(jnp.float32)
            factors[member, :EDGE] = factor[:EDGE, here]
            factors[member, EDGE:] = factor[columns - EDGE:, here]
    rows = lax.broadcasted_iota(jnp.int32, (EDGE, levels), 0)
    total[...] = summed
    total[:EDGE] = jnp.where(rows < SWEEPS, 0.0, summed[:EDGE])
    total[columns - EDGE:] = jnp.where(rows >= EDGE - SWEEPS, 0.0, summed[columns - EDGE:])
    owned = columns // owners
    for chip in range(owners // 2):
        here = pl.multiple_of((2 * chip + core[0]) * owned, owned)
        there = pl.multiple_of((2 * chip + 1 - core[0]) * owned, owned)
        keep[chip * owned:(chip + 1) * owned] = total[pl.ds(here, owned)]
        send[chip * owned:(chip + 1) * owned] = total[pl.ds(there, owned)]


def edge_kernel(ends, factors, low, high, edges):
    members, _, levels = ends.shape
    windows = []
    for member in range(members):
        windows += [low[member], ends[member], high[member]]
    field = swept(jnp.concatenate(windows, axis=0))
    size = 4 * EDGE
    start = jnp.zeros((EDGE, levels), jnp.float32)
    stop = start
    for member in range(members):
        base = size * member + EDGE
        start = start + field[base:base + EDGE] * factors[member, :EDGE]
        stop = stop + field[base + EDGE:base + 2 * EDGE] * factors[member, EDGE:]
    rows = lax.broadcasted_iota(jnp.int32, (EDGE, levels), 0)
    edges[:EDGE] = jnp.where(rows < SWEEPS, start, 0.0)
    edges[EDGE:] = jnp.where(rows >= EDGE - SWEEPS, stop, 0.0)


def member_sum(control, perturb, core, owners):
    members, columns, levels = control.shape
    low, high = edge_columns(control, "sub")
    ends = pltpu.VMEM((members, 2 * EDGE, levels), jnp.float32)
    half = pltpu.VMEM((columns // 2, levels), jnp.float32)
    keep, send, fields, factors = pl.pallas_call(
        functools.partial(inside_kernel, owners=owners),
        out_shape=(half, half, ends, ends),
        in_specs=[pl.BlockSpec(memory_space=pltpu.SMEM)] + [pl.BlockSpec(memory_space=pltpu.HBM)] * 2,
        out_specs=(ON_CHIP,) * 4,
        scratch_shapes=[
            pltpu.VMEM((columns, members * levels), control.dtype),
            pltpu.VMEM((columns, members * levels), perturb.dtype),
            pltpu.VMEM((columns, levels), jnp.float32),
            pltpu.SemaphoreType.DMA((2, members)),
        ],
        compiler_params=room(16),
        name="inside",
    )(core, *(pltpu.with_memory_space_constraint(a, pltpu.HBM) for a in (control, perturb)))
    edges = pl.pallas_call(
        edge_kernel,
        out_shape=pltpu.VMEM((2 * EDGE, levels), jnp.float32),
        in_specs=[ON_CHIP] * 4,
        out_specs=ON_CHIP,
        compiler_params=room(16),
        name="edges",
    )(*near(fields, factors, low, high))
    return keep, send, edges


def bit_swap(block, axis, bit):
    count = lax.axis_size(axis)
    return lax.ppermute(block, axis, [(i, i ^ bit) for i in range(count)])


def pick(block, dim, which):
    return lax.squeeze(lax.dynamic_slice_in_dim(block, which, 1, dim), (dim,))


def reduce_pairs(keep, send, edges, layouts, axis):
    count = lax.axis_size(axis)
    arrived = bit_swap(send, axis, 1)
    mine = jnp.concatenate([keep + arrived, edges], axis=0)
    if count <= 8:
        parts = [bit_swap(mine, axis, bit) for bit in range(2, count, 2)]
        for part in parts:
            mine = mine + part
    else:
        for step in range(1, count.bit_length() - 1):
            mine = mine + bit_swap(mine, axis, 1 << step)
    mine, layouts = lax.optimization_barrier((mine, layouts))
    return mine, bit_swap(mine, axis, 1), layouts


def scatter_pairs(keep, send, axis):
    count = lax.axis_size(axis)
    me = lax.axis_index(axis)
    block = keep + bit_swap(send, axis, 1)
    block = block.reshape((count // 2, -1) + block.shape[1:])
    if count <= 8:
        chip = me >> 1
        bits = list(range(1, count // 2))
        parts = [bit_swap(pick(block, 0, chip ^ bit), axis, 2 * bit) for bit in bits[-1:] + bits[:-1]]
        owned = pick(block, 0, chip)
        for part in parts:
            owned = owned + part
        return owned
    for step in range(1, count.bit_length() - 1):
        side = (me >> step) & 1
        halves = block.reshape((-1, 2) + block.shape[1:])
        block = pick(halves, 1, side) + bit_swap(pick(halves, 1, 1 - side), axis, 1 << step)
    return block.reshape(block.shape[1:])


def layout_kernel(count, indices, weights, by_column, by_slot, spread):
    columns, slots = by_column.shape
    lanes = spread.shape[1]
    row = indices[...]
    picked = (lax.broadcasted_iota(jnp.int32, (columns, slots), 0) == row).astype(jnp.float32)
    by_column[...] = picked.astype(jnp.bfloat16)
    by_slot[...] = jnp.transpose(picked).astype(jnp.bfloat16)
    live = lax.broadcasted_iota(jnp.int32, (1, slots), 1) < count[0, 0]
    spread[...] = jnp.transpose(jnp.broadcast_to(jnp.where(live, weights[...], 0.0), (lanes, slots)))


def layout_call(count, indices, weights, columns, lanes):
    slots = indices.shape[1]
    return pl.pallas_call(
        layout_kernel,
        out_shape=(
            pltpu.VMEM((columns, slots), jnp.bfloat16),
            pltpu.VMEM((slots, columns), jnp.bfloat16),
            pltpu.VMEM((slots, lanes), jnp.float32),
        ),
        in_specs=[pl.BlockSpec(memory_space=pltpu.SMEM)] + [ON_CHIP] * 2,
        out_specs=(ON_CHIP,) * 3,
        compiler_params=room(16),
        name="layout",
    )(count, *near(indices, weights))


def observe_kernel(
    core, mine, other, by_column, by_slot, spread, background, targets, w_in, b_in, w_out, keep, send, whole, slope, *, scale, block, chunk
):
    slots, levels = background.shape
    half_columns = mine.shape[0] - 2 * EDGE
    hidden = w_in.shape[1]
    edges = mine[half_columns:] + other[half_columns:]
    first = edges[:EDGE]
    last = edges[EDGE:]
    even = core[0] == 0
    none = jnp.zeros_like(first)
    parts = []
    for rows, low, high in ((mine, even, ~even), (other, ~even, even)):
        parts += [
            rows[:EDGE] + jnp.where(low, first, none),
            rows[EDGE:half_columns - EDGE],
            rows[half_columns - EDGE:half_columns] + jnp.where(high, last, none),
        ]
    increment = jnp.concatenate(parts, axis=0) * scale
    whole[...] = increment[:half_columns]
    top = increment.astype(jnp.bfloat16)
    rest = (increment - top.astype(jnp.float32)).astype(jnp.bfloat16)
    table = jnp.concatenate([top, rest], axis=1)
    half_bias = 0.5 * b_in[...]

    def start(index):
        base = index * block
        pair = jnp.dot(by_slot[base:base + block, :], table, preferred_element_type=jnp.float32)
        sampled = pair[:, :levels] + pair[:, levels:]
        inputs = 0.5 * (background[base:base + block, :].astype(jnp.float32) + sampled).astype(jnp.bfloat16)
        return dict(base=base, slot=index % 2, inputs=inputs, outputs=None, back=None)

    def forward(st, c):
        sl = slice(c, c + chunk)
        half = jnp.dot(st["inputs"], w_in[:, sl], preferred_element_type=jnp.float32) + half_bias[0:1, sl]
        square = half * half
        bend = jnp.tanh(half * (2.0 * GELU_ROOT + 8.0 * GELU_ROOT * GELU_CUBE * square))
        lift = 1.0 + bend
        st_hidden = (half * lift).astype(jnp.bfloat16)
        rise = GELU_ROOT + 12.0 * GELU_ROOT * GELU_CUBE * square
        tilt = lift * (0.5 + half * ((1.0 - bend) * rise))
        slope[st["slot"], :, sl] = tilt
        part = jnp.dot(st_hidden, w_out[sl, :], preferred_element_type=jnp.float32)
        st["outputs"] = part if st["outputs"] is None else st["outputs"] + part

    def middle(st):
        base = st["base"]
        col = spread[base:base + block, :]
        st["misfit"] = ((st["outputs"] - targets[base:base + block, :].astype(jnp.float32)) * col).astype(jnp.bfloat16)

    def backward(st, c):
        sl = slice(c, c + chunk)
        back = lax.dot_general(st["misfit"], w_out[sl, :], (((1,), (1,)), ((), ())), preferred_element_type=jnp.float32)
        back = (back * slope[st["slot"], :, sl]).astype(jnp.bfloat16)
        part = lax.dot_general(back, w_in[:, sl], (((1,), (1,)), ((), ())), preferred_element_type=jnp.float32)
        st["back"] = part if st["back"] is None else st["back"] + part

    def finish(st, total):
        picked = by_column[:, st["base"]:st["base"] + block]
        part = jnp.dot(picked, st["back"].astype(jnp.bfloat16), preferred_element_type=jnp.float32)
        return part if total is None else total + part

    blocks = slots // block
    total = None
    behind = None
    for index in range(blocks + 1):
        ahead = start(index) if index < blocks else None
        for c in range(0, hidden, chunk):
            if ahead is not None:
                forward(ahead, c)
            if behind is not None:
                backward(behind, c)
        if behind is not None:
            total = finish(behind, total)
        if ahead is not None:
            middle(ahead)
        behind = ahead
    keep[...] = total[:half_columns]
    send[...] = total[half_columns:]


def largest_part(size, limit):
    part = min(size, limit)
    while size % part:
        part -= 1
    return part


def observe_call(core, mine, other, by_column, by_slot, spread, background, targets, w_in, b_in, w_out, scale):
    block = largest_part(background.shape[0], 512)
    chunk = largest_part(w_in.shape[1], 256)
    half = pltpu.VMEM((mine.shape[0] - 2 * EDGE, mine.shape[1]), jnp.float32)
    return pl.pallas_call(
        functools.partial(observe_kernel, scale=scale, block=block, chunk=chunk),
        out_shape=(half,) * 3,
        in_specs=[pl.BlockSpec(memory_space=pltpu.SMEM)] + [ON_CHIP] * 10,
        out_specs=(ON_CHIP,) * 3,
        scratch_shapes=[pltpu.VMEM((2, block, w_in.shape[1]), jnp.float32)],
        compiler_params=room(32),
        name="observe",
    )(core, *near(mine, other, by_column, by_slot, spread, background, targets, w_in, b_in, w_out))


def per_device(
    control,
    perturb,
    obs_column,
    obs_count,
    obs_background,
    obs_value,
    obs_weight,
    w_in,
    b_in,
    w_out,
):
    members = perturb.shape[0] * lax.axis_size("mem")
    scale = (members - 1) ** (-0.5)
    count = lax.axis_size("mem")
    me = lax.axis_index("mem")
    columns = control.shape[1]
    owned = columns // count
    indices = obs_column.reshape(1, -1)
    slots = indices.shape[1]
    paired = count > 1 and count & (count - 1) == 0
    core = (me & 1 if paired else jnp.int32(0)).reshape(1)
    keep, send, edges = member_sum(control, perturb, core, count if paired else 2)
    if paired:
        owner = indices // owned
        side = ((owner ^ me) & 1) * (columns // 2)
        indices = side + (owner // 2) * owned + indices % owned
    layouts = layout_call(obs_count, indices, obs_weight.reshape(1, slots), columns, obs_value.shape[-1])
    if paired:
        mine, other, layouts = reduce_pairs(keep, send, edges, layouts, "mem")
    else:
        mine = lax.psum(jnp.concatenate([keep, edges], axis=0), "mem")
        other = jnp.pad(lax.psum(send, "mem"), ((0, edges.shape[0]), (0, 0)))
    keep, send, whole = observe_call(
        core,
        mine,
        other,
        *layouts,
        obs_background.reshape(slots, -1),
        obs_value.reshape(slots, -1),
        w_in,
        b_in.reshape(1, -1),
        w_out,
        scale,
    )
    if paired:
        increment = pick(whole.reshape(count // 2, owned, -1), 0, me // 2)
        grad_columns = scatter_pairs(keep, send, "mem")
    else:
        halo = mine[columns // 2 :]
        full = jnp.concatenate([mine[: columns // 2], other[: columns // 2]], axis=0)
        full = full.at[:EDGE].add(halo[:EDGE]).at[-EDGE:].add(halo[EDGE:])
        increment = lax.dynamic_slice_in_dim(full, me * owned, owned, 0) * scale
        gradient = jnp.concatenate([keep, send], axis=0)
        grad_columns = lax.psum_scatter(gradient, "mem", scatter_dimension=0, tiled=True)
    return (increment, grad_columns)


def solution(mesh):
    return jax.shard_map(
        per_device,
        mesh=mesh,
        in_specs=(
            P("mem", "sub", None),
            P("mem", "sub", None),
            P("mem", "sub", None),
            P("mem", "sub"),
            P("mem", "sub", None, None),
            P("mem", "sub", None, None),
            P("mem", "sub", None),
            P(),
            P(),
            P(),
        ),
        out_specs=(P(("sub", "mem"), None), P(("sub", "mem"), None)),
        check_vma=False,
    )
```

```python
import functools

import jax
import jax.numpy as jnp
from jax import lax
from jax.experimental import pallas as pl
from jax.experimental.pallas import tpu as pltpu
from jax.sharding import PartitionSpec as P

SWEEPS = 4


diffusion = 0.4
GELU_ROOT = 0.7978845608028654
GELU_CUBE = 0.044715

ON_CHIP = pl.BlockSpec(memory_space=pltpu.VMEM)
EDGE = 8 * -(-2 * SWEEPS // 8)


def near(*arrays):
    return [pltpu.with_memory_space_constraint(a, pltpu.VMEM) for a in arrays]


def room(mebibytes):
    return pltpu.CompilerParams(vmem_limit_bytes=mebibytes << 20)


def edge_columns(block, axis):
    count = lax.axis_size(axis)
    forward = [(i, (i + 1) % count) for i in range(count)]
    backward = [(target, source) for source, target in forward]
    first = block[:, :EDGE].astype(jnp.float32)
    last = block[:, -EDGE:].astype(jnp.float32)
    low = lax.ppermute(last, axis, forward)
    high = lax.ppermute(first, axis, backward)
    return low, high


def swept(field):
    rows = field.shape[0]
    for _ in range(SWEEPS):
        low = pltpu.roll(field, 1, 0)
        high = pltpu.roll(field, rows - 1, 0)
        field = field + diffusion * ((low - 2.0 * field) + high)
    return field


def stencil_matrix(columns):
    taps = [1.0]
    for _ in range(SWEEPS):
        wide = [0.0] + taps + [0.0]
        taps = [
            (1.0 - 2.0 * diffusion) * wide[i]
            + diffusion * ((wide[i - 1] if i else 0.0) + (wide[i + 1] if i + 1 < len(wide) else 0.0))
            for i in range(len(wide))
        ]
    row = lax.broadcasted_iota(jnp.int32, (columns, columns), 0)
    apart = jnp.abs(row - lax.broadcasted_iota(jnp.int32, (columns, columns), 1))
    matrix = jnp.zeros((columns, columns), jnp.float32)
    for distance in range(SWEEPS + 1):
        matrix = jnp.where(apart == distance, taps[SWEEPS + distance], matrix)
    top = matrix.astype(jnp.bfloat16)
    return top, (matrix - top.astype(jnp.float32)).astype(jnp.bfloat16)


def inside_kernel(core, control, perturb, keep, send, ends, factors, fields, weights, total, arrived, *, owners):
    members, columns, levels = control.shape
    copies = []
    for member in range(members):
        lanes = slice(member * levels, (member + 1) * levels)
        copies.append((
            pltpu.make_async_copy(control.at[member], fields.at[:, lanes], arrived.at[0, member]),
            pltpu.make_async_copy(perturb.at[member], weights.at[:, lanes], arrived.at[1, member]),
        ))
    for pair in copies:
        for copy in pair:
            copy.start()
    top, rest = stencil_matrix(columns)
    summed = None
    group = 2 if members % 2 == 0 else 1
    for first in range(0, members, group):
        for member in range(first, first + group):
            for copy in copies[member]:
                copy.wait()
        lanes = slice(first * levels, (first + group) * levels)
        field = fields[:, lanes]
        factor = weights[:, lanes].astype(jnp.float32)
        local = jnp.dot(top, field, preferred_element_type=jnp.float32)
        local = local + jnp.dot(rest, field, preferred_element_type=jnp.float32)
        product = local * factor
        for step in range(group):
            here = slice(step * levels, (step + 1) * levels)
            summed = product[:, here] if summed is None else summed + product[:, here]
            member = first + step
            ends[member, :EDGE] = field[:EDGE, here].astype(jnp.float32)
            ends[member, EDGE:] = field[columns - EDGE:, here].astype(jnp.float32)
            factors[member, :EDGE] = factor[:EDGE, here]
            factors[member, EDGE:] = factor[columns - EDGE:, here]
    rows = lax.broadcasted_iota(jnp.int32, (EDGE, levels), 0)
    total[...] = summed
    total[:EDGE] = jnp.where(rows < SWEEPS, 0.0, summed[:EDGE])
    total[columns - EDGE:] = jnp.where(rows >= EDGE - SWEEPS, 0.0, summed[columns - EDGE:])
    owned = columns // owners
    for chip in range(owners // 2):
        here = pl.multiple_of((2 * chip + core[0]) * owned, owned)
        there = pl.multiple_of((2 * chip + 1 - core[0]) * owned, owned)
        keep[chip * owned:(chip + 1) * owned] = total[pl.ds(here, owned)]
        send[chip * owned:(chip + 1) * owned] = total[pl.ds(there, owned)]


def edge_kernel(ends, factors, low, high, edges):
    members, _, levels = ends.shape
    windows = []
    for member in range(members):
        windows += [low[member], ends[member], high[member]]
    field = swept(jnp.concatenate(windows, axis=0))
    size = 4 * EDGE
    start = jnp.zeros((EDGE, levels), jnp.float32)
    stop = start
    for member in range(members):
        base = size * member + EDGE
        start = start + field[base:base + EDGE] * factors[member, :EDGE]
        stop = stop + field[base + EDGE:base + 2 * EDGE] * factors[member, EDGE:]
    rows = lax.broadcasted_iota(jnp.int32, (EDGE, levels), 0)
    edges[...] = jnp.where(rows < SWEEPS, start, jnp.where(rows >= EDGE - SWEEPS, stop, 0.0))


def member_sum(control, perturb, core, owners):
    members, columns, levels = control.shape
    low, high = edge_columns(control, "sub")
    ends = pltpu.VMEM((members, 2 * EDGE, levels), jnp.float32)
    half = pltpu.VMEM((columns // 2, levels), jnp.float32)
    keep, send, fields, factors = pl.pallas_call(
        functools.partial(inside_kernel, owners=owners),
        out_shape=(half, half, ends, ends),
        in_specs=[pl.BlockSpec(memory_space=pltpu.SMEM)] + [pl.BlockSpec(memory_space=pltpu.HBM)] * 2,
        out_specs=(ON_CHIP,) * 4,
        scratch_shapes=[
            pltpu.VMEM((columns, members * levels), control.dtype),
            pltpu.VMEM((columns, members * levels), perturb.dtype),
            pltpu.VMEM((columns, levels), jnp.float32),
            pltpu.SemaphoreType.DMA((2, members)),
        ],
        compiler_params=room(16),
        name="inside",
    )(core, *(pltpu.with_memory_space_constraint(a, pltpu.HBM) for a in (control, perturb)))
    edges = pl.pallas_call(
        edge_kernel,
        out_shape=pltpu.VMEM((EDGE, levels), jnp.float32),
        in_specs=[ON_CHIP] * 4,
        out_specs=ON_CHIP,
        compiler_params=room(16),
        name="edges",
    )(*near(fields, factors, low, high))
    return keep, send, edges


def bit_swap(block, axis, bit):
    count = lax.axis_size(axis)
    return lax.ppermute(block, axis, [(i, i ^ bit) for i in range(count)])


def pick(block, dim, which):
    return lax.squeeze(lax.dynamic_slice_in_dim(block, which, 1, dim), (dim,))


def reduce_pairs(keep, send, edges, layouts, axis):
    count = lax.axis_size(axis)
    arrived = bit_swap(send, axis, 1)
    mine = jnp.concatenate([keep + arrived, edges], axis=0)
    if count <= 8:
        parts = [bit_swap(mine, axis, bit) for bit in range(2, count, 2)]
        for part in parts:
            mine = mine + part
    else:
        for step in range(1, count.bit_length() - 1):
            mine = mine + bit_swap(mine, axis, 1 << step)
    mine, layouts = lax.optimization_barrier((mine, layouts))
    return mine, bit_swap(mine, axis, 1), layouts


def scatter_pairs(keep, send, axis):
    count = lax.axis_size(axis)
    me = lax.axis_index(axis)
    block = keep + bit_swap(send, axis, 1)
    block = block.reshape((count // 2, -1) + block.shape[1:])
    if count <= 8:
        chip = me >> 1
        bits = list(range(1, count // 2))
        parts = [bit_swap(pick(block, 0, chip ^ bit), axis, 2 * bit) for bit in bits[-1:] + bits[:-1]]
        owned = pick(block, 0, chip)
        for part in parts:
            owned = owned + part
        return owned
    for step in range(1, count.bit_length() - 1):
        side = (me >> step) & 1
        halves = block.reshape((-1, 2) + block.shape[1:])
        block = pick(halves, 1, side) + bit_swap(pick(halves, 1, 1 - side), axis, 1 << step)
    return block.reshape(block.shape[1:])


def layout_kernel(count, indices, weights, by_column, by_slot, spread):
    columns, slots = by_column.shape
    lanes = spread.shape[1]
    row = indices[...]
    picked = (lax.broadcasted_iota(jnp.int32, (columns, slots), 0) == row).astype(jnp.float32)
    by_column[...] = picked.astype(jnp.bfloat16)
    by_slot[...] = jnp.transpose(picked).astype(jnp.bfloat16)
    live = lax.broadcasted_iota(jnp.int32, (1, slots), 1) < count[0, 0]
    spread[...] = jnp.transpose(jnp.broadcast_to(jnp.where(live, weights[...], 0.0), (lanes, slots)))


def layout_call(count, indices, weights, columns, lanes):
    slots = indices.shape[1]
    return pl.pallas_call(
        layout_kernel,
        out_shape=(
            pltpu.VMEM((columns, slots), jnp.bfloat16),
            pltpu.VMEM((slots, columns), jnp.bfloat16),
            pltpu.VMEM((slots, lanes), jnp.float32),
        ),
        in_specs=[pl.BlockSpec(memory_space=pltpu.SMEM)] + [ON_CHIP] * 2,
        out_specs=(ON_CHIP,) * 3,
        compiler_params=room(16),
        name="layout",
    )(count, *near(indices, weights))


def observe_kernel(
    core, mine, other, by_column, by_slot, spread, background, targets, w_in, b_in, w_out, keep, send, whole, slope, *, scale, block, chunk
):
    slots, levels = background.shape
    half_columns = mine.shape[0] - EDGE
    hidden = w_in.shape[1]
    edges = mine[half_columns:] + other[half_columns:]
    place = lax.broadcasted_iota(jnp.int32, edges.shape, 0)
    none = jnp.zeros_like(edges)
    first = jnp.where(place < SWEEPS, edges, none)
    last = jnp.where(place >= EDGE - SWEEPS, edges, none)
    even = core[0] == 0
    parts = []
    for rows, low, high in ((mine, even, ~even), (other, ~even, even)):
        parts += [
            rows[:EDGE] + jnp.where(low, first, none),
            rows[EDGE:half_columns - EDGE],
            rows[half_columns - EDGE:half_columns] + jnp.where(high, last, none),
        ]
    increment = jnp.concatenate(parts, axis=0) * scale
    whole[...] = increment[:half_columns]
    top = increment.astype(jnp.bfloat16)
    rest = (increment - top.astype(jnp.float32)).astype(jnp.bfloat16)
    table = jnp.concatenate([top, rest], axis=1)
    half_bias = 0.5 * b_in[...]

    def start(index):
        base = index * block
        pair = jnp.dot(by_slot[base:base + block, :], table, preferred_element_type=jnp.float32)
        sampled = pair[:, :levels] + pair[:, levels:]
        inputs = 0.5 * (background[base:base + block, :].astype(jnp.float32) + sampled).astype(jnp.bfloat16)
        return dict(base=base, slot=index % 2, inputs=inputs, outputs=None, back=None)

    def forward(st, c):
        sl = slice(c, c + chunk)
        half = jnp.dot(st["inputs"], w_in[:, sl], preferred_element_type=jnp.float32) + half_bias[0:1, sl]
        square = half * half
        bend = jnp.tanh(half * (2.0 * GELU_ROOT + 8.0 * GELU_ROOT * GELU_CUBE * square))
        lift = 1.0 + bend
        st_hidden = (half * lift).astype(jnp.bfloat16)
        rise = GELU_ROOT + 12.0 * GELU_ROOT * GELU_CUBE * square
        tilt = lift * (0.5 + half * ((1.0 - bend) * rise))
        slope[st["slot"], :, sl] = tilt
        part = jnp.dot(st_hidden, w_out[sl, :], preferred_element_type=jnp.float32)
        st["outputs"] = part if st["outputs"] is None else st["outputs"] + part

    def middle(st):
        base = st["base"]
        col = spread[base:base + block, :]
        st["misfit"] = ((st["outputs"] - targets[base:base + block, :].astype(jnp.float32)) * col).astype(jnp.bfloat16)

    def backward(st, c):
        sl = slice(c, c + chunk)
        back = lax.dot_general(st["misfit"], w_out[sl, :], (((1,), (1,)), ((), ())), preferred_element_type=jnp.float32)
        back = (back * slope[st["slot"], :, sl]).astype(jnp.bfloat16)
        part = lax.dot_general(back, w_in[:, sl], (((1,), (1,)), ((), ())), preferred_element_type=jnp.float32)
        st["back"] = part if st["back"] is None else st["back"] + part

    def finish(st, total):
        picked = by_column[:, st["base"]:st["base"] + block]
        part = jnp.dot(picked, st["back"].astype(jnp.bfloat16), preferred_element_type=jnp.float32)
        return part if total is None else total + part

    blocks = slots // block
    total = None
    behind = None
    for index in range(blocks + 1):
        ahead = start(index) if index < blocks else None
        for c in range(0, hidden, chunk):
            if ahead is not None:
                forward(ahead, c)
            if behind is not None:
                backward(behind, c)
        if behind is not None:
            total = finish(behind, total)
        if ahead is not None:
            middle(ahead)
        behind = ahead
    keep[...] = total[:half_columns]
    send[...] = total[half_columns:]


def largest_part(size, limit):
    part = min(size, limit)
    while size % part:
        part -= 1
    return part


def observe_call(core, mine, other, by_column, by_slot, spread, background, targets, w_in, b_in, w_out, scale):
    block = largest_part(background.shape[0], 512)
    chunk = largest_part(w_in.shape[1], 256)
    half = pltpu.VMEM((mine.shape[0] - EDGE, mine.shape[1]), jnp.float32)
    return pl.pallas_call(
        functools.partial(observe_kernel, scale=scale, block=block, chunk=chunk),
        out_shape=(half,) * 3,
        in_specs=[pl.BlockSpec(memory_space=pltpu.SMEM)] + [ON_CHIP] * 10,
        out_specs=(ON_CHIP,) * 3,
        scratch_shapes=[pltpu.VMEM((2, block, w_in.shape[1]), jnp.float32)],
        compiler_params=room(32),
        name="observe",
    )(core, *near(mine, other, by_column, by_slot, spread, background, targets, w_in, b_in, w_out))


def per_device(
    control,
    perturb,
    obs_column,
    obs_count,
    obs_background,
    obs_value,
    obs_weight,
    w_in,
    b_in,
    w_out,
):
    members = perturb.shape[0] * lax.axis_size("mem")
    scale = (members - 1) ** (-0.5)
    count = lax.axis_size("mem")
    me = lax.axis_index("mem")
    columns = control.shape[1]
    owned = columns // count
    indices = obs_column.reshape(1, -1)
    slots = indices.shape[1]
    paired = count > 1 and count & (count - 1) == 0
    core = (me & 1 if paired else jnp.int32(0)).reshape(1)
    keep, send, edges = member_sum(control, perturb, core, count if paired else 2)
    if paired:
        owner = indices // owned
        side = ((owner ^ me) & 1) * (columns // 2)
        indices = side + (owner // 2) * owned + indices % owned
    layouts = layout_call(obs_count, indices, obs_weight.reshape(1, slots), columns, obs_value.shape[-1])
    if paired:
        mine, other, layouts = reduce_pairs(keep, send, edges, layouts, "mem")
    else:
        mine = lax.psum(jnp.concatenate([keep, edges], axis=0), "mem")
        other = jnp.pad(lax.psum(send, "mem"), ((0, edges.shape[0]), (0, 0)))
    keep, send, whole = observe_call(
        core,
        mine,
        other,
        *layouts,
        obs_background.reshape(slots, -1),
        obs_value.reshape(slots, -1),
        w_in,
        b_in.reshape(1, -1),
        w_out,
        scale,
    )
    if paired:
        increment = pick(whole.reshape(count // 2, owned, -1), 0, me // 2)
        grad_columns = scatter_pairs(keep, send, "mem")
    else:
        halo = mine[columns // 2 :]
        full = jnp.concatenate([mine[: columns // 2], other[: columns // 2]], axis=0)
        full = full.at[:SWEEPS].add(halo[:SWEEPS]).at[-SWEEPS:].add(halo[EDGE - SWEEPS :])
        increment = lax.dynamic_slice_in_dim(full, me * owned, owned, 0) * scale
        gradient = jnp.concatenate([keep, send], axis=0)
        grad_columns = lax.psum_scatter(gradient, "mem", scatter_dimension=0, tiled=True)
    return (increment, grad_columns)


def solution(mesh):
    return jax.shard_map(
        per_device,
        mesh=mesh,
        in_specs=(
            P("mem", "sub", None),
            P("mem", "sub", None),
            P("mem", "sub", None),
            P("mem", "sub"),
            P("mem", "sub", None, None),
            P("mem", "sub", None, None),
            P("mem", "sub", None),
            P(),
            P(),
            P(),
        ),
        out_specs=(P(("sub", "mem"), None), P(("sub", "mem"), None)),
        check_vma=False,
    )
```
